32 devices in a mesh: clip: 2 (over x), tm: 16 (over z, y, core).
Axes of the slice: x: 2, y: 2, z: 4, core: 2. Of those that a mesh axis runs over, the one named last changes fastest.
Arguments:
- frames: bfloat16 [64, 1024, 256], P('tm', 'clip'), parts along dimension 1, may hold values from -6 to 6
- gain_one: float32 [256], replicated, may hold values from 0.25 to 1.75
- conv_one: bfloat16 [3, 3, 3, 256, 256], replicated, may hold values from -0.078125 to 0.078125
- gain_two: float32 [256], replicated, may hold values from 0.25 to 1.75
- conv_two: bfloat16 [3, 3, 3, 256, 256], replicated, may hold values from -0.078125 to 0.078125
- out_weight: bfloat16 [256, 256], replicated, may hold values from -0.375 to 0.375
Outputs:
- latent: bfloat16 [64, 1024, 256], P(None, ('clip', 'tm')), parts along dimension 1
The draws below stay inside these ranges and needn't reach their ends.
There are 2 independent parts, one for each index of `clip`. The reference program is written for one: setup_inputs(seed, part) draws one part's arguments, and reference() takes and returns one part's arrays. A program takes and returns all parts, laid end to end along the dimension named above; an argument that names none is the same for every part. Nothing has to cross between parts.
All inputs are finite; a program needn't handle non-finite values.
Results may differ from the reference program's by a relative error of at most 0.0065.
Values may be sent and summed in bfloat16 or wider, within the bound.
A program may use at most 192 MiB of HBM per device.

```python
import jax
import jax.numpy as jnp
from jax import lax

C = 256
ROWS = 4
COLS = 128
CELLS = 512
FRAMES = 64


def levels(rng, dims, split, low, largest):
    def one(axis_at, shards_of):
        steps = jax.random.uniform(jax.random.fold_in(jax.random.fold_in(rng, 6), axis_at), (shards_of,), jnp.float32, low / len(split), largest / len(split))
        return jnp.repeat(jnp.exp(steps), dims[axis_at] // shards_of).reshape((-1,) + (1,) * (len(dims) - axis_at - 1))

    factor_of = one(*split[0])
    for cut in split[1:]:
        factor_of = factor_of * one(*cut)
    return factor_of


def bell_draw(stream_key, shape, width, limit, cuts=(), kind=jnp.bfloat16):
    values = width * jax.random.normal(stream_key, shape, jnp.float32)
    if cuts:
        values = values * levels(stream_key, shape, cuts, -0.22, 0.18)
    return jnp.clip(values, -limit, limit).astype(kind)


def setup_inputs(seed: int = 0, part: int = 0) -> dict:
    arg_keys = jax.random.split(jax.random.key(seed), 7)
    part_splits = jax.random.split(jax.random.fold_in(arg_keys[6], part), 7)
    return {
        "frames": bell_draw(part_splits[0], (FRAMES, CELLS, C), 1.0, 6.0, ((0, 16),)),
        "gain_one": jnp.clip(1.0 + 0.15 * jax.random.normal(arg_keys[1], (C,), jnp.float32), 0.25, 1.75),
        "conv_one": bell_draw(arg_keys[2], (3, 3, 3, C, C), (27 * C) ** -0.5, 0.078125),
        "gain_two": jnp.clip(1.0 + 0.15 * jax.random.normal(arg_keys[3], (C,), jnp.float32), 0.25, 1.75),
        "conv_two": bell_draw(arg_keys[4], (3, 3, 3, C, C), (27 * C) ** -0.5, 0.078125),
        "out_weight": bell_draw(arg_keys[5], (C, C), C ** -0.5, 0.375),
    }


def norm_act(x, gain):
    values = x.astype(jnp.float32)
    scale = lax.rsqrt(lax.optimization_barrier(jnp.mean(values * values, axis=-1, keepdims=True)) + 1e-06)
    return jax.nn.silu(values * scale * gain).astype(jnp.bfloat16)

def causal_conv(act, kernel):
    frame_count = act.shape[0]
    channels = act.shape[-1]
    grid = act.reshape(frame_count, ROWS, COLS, channels)
    padded = jnp.pad(grid, ((2, 0), (1, 1), (1, 1), (0, 0)))
    total = jnp.zeros((frame_count * ROWS * COLS, channels), jnp.float32)
    for tap_t in range(3):
        for tap_r in range(3):
            for tap_c in range(3):
                slab = padded[tap_t:tap_t + frame_count, tap_r:tap_r + ROWS, tap_c:tap_c + COLS, :]
                total = total + jnp.dot(slab.reshape(-1, channels), kernel[tap_t, tap_r, tap_c], preferred_element_type=jnp.float32)
    return total.reshape(frame_count, ROWS * COLS, channels)

def block(x, gain, kernel):
    act = norm_act(x, gain)
    return (x.astype(jnp.float32) + causal_conv(act, kernel)).astype(jnp.bfloat16)

def reference(frames, gain_one, conv_one, gain_two, conv_two, out_weight):
    first = block(frames, gain_one, conv_one)
    second = block(first, gain_two, conv_two)
    channels = second.shape[-1]
    latent = jnp.dot(second.reshape(-1, channels), out_weight, preferred_element_type=jnp.float32)
    return latent.reshape(second.shape).astype(jnp.bfloat16)
```

```python
import functools

import jax
import jax.numpy as jnp
from jax import lax
from jax.experimental import pallas as pl
from jax.experimental.pallas import tpu as pltpu
from jax.sharding import PartitionSpec as P

ROWS = 4
COLS = 128
MESH = pl.DeviceIdType.MESH


def norm_act(x, gain):
    values = x.astype(jnp.float32)
    scale = lax.rsqrt(jnp.mean(values * values, axis=-1, keepdims=True) + 1e-06)
    scaled = values * scale * gain
    return scaled * (0.5 * jnp.tanh(0.5 * scaled) + 0.5)


def store_shifted(acts, frame, row, act):
    channels = act.shape[-1]
    place = lax.broadcasted_iota(jnp.int32, act.shape, 0)
    before = jnp.where(place == 0, 0.0, pltpu.roll(act, 1, 0))
    after = jnp.where(place == COLS - 1, 0.0, pltpu.roll(act, COLS - 1, 0))
    acts[frame, row, :, :channels] = before.astype(jnp.bfloat16)
    acts[frame, row, :, channels : 2 * channels] = act.astype(jnp.bfloat16)
    acts[frame, row, :, 2 * channels :] = after.astype(jnp.bfloat16)


def conv_row(acts, kernel, frame, source, tap, rows):
    total = None
    for tap_t in range(3):
        for at in range(rows):
            window = acts[pl.ds(frame + tap_t, 2), source + at]
            part = jnp.dot(
                window.reshape(2 * COLS, window.shape[-1]),
                kernel[tap_t * 3 + tap + at],
                preferred_element_type=jnp.float32,
            )
            total = part if total is None else total + part
    return total.reshape(2, COLS, total.shape[-1])


def both_rows(acts, kernel, frame, half):
    border = conv_row(acts, kernel, frame, 2 * half, 1 - half, 2)
    inner = conv_row(acts, kernel, frame, half, 0, 3)
    return (((ROWS - 1) * half, border), (1 + half, inner))


def fused(
    n,
    frames_ref,
    gain_one,
    conv_one,
    gain_two,
    conv_two,
    out_weight,
    out_ref,
    frames,
    halo_one,
    halo_two,
    edge_two,
    kernel_one,
    kernel_two,
    project,
    acts_one,
    acts_two,
    first,
    result,
    load_sems,
    halo_send,
    halo_recv,
    edge_send,
    edge_recv,
    out_send,
    out_recv,
    own_sem,
):
    me = lax.axis_index("tm")
    count = frames.shape[0]
    channels = frames.shape[-1]
    owned = result.shape[2]
    per_row = COLS // owned
    earlier = me - 1
    later = me + 1

    loads = [pltpu.make_async_copy(frames_ref, frames, load_sems.at[0])]
    for source, target in ((conv_one, kernel_one), (conv_two, kernel_two)):
        for tap in range(9):
            sem = load_sems.at[len(loads)]
            loads.append(pltpu.make_async_copy(source.at[tap], target.at[tap], sem))
    loads.append(pltpu.make_async_copy(out_weight, project, load_sems.at[19]))
    for load in loads[:10]:
        load.start()

    barrier = pltpu.get_barrier_semaphore()

    @pl.loop(1, n)
    def _(step):
        pl.semaphore_signal(
            barrier, inc=1, device_id={"tm": lax.rem(me + step, n)}, device_id_type=MESH
        )

    loads[0].wait()

    @pl.loop(0, count * ROWS)
    def _(index):
        frame = index // ROWS
        row = index % ROWS
        act = norm_act(frames[frame, row], gain_one[...])
        store_shifted(acts_one, frame + 2, row, act)

    pl.semaphore_wait(barrier, n - 1)

    halo_copy = pltpu.make_async_remote_copy(
        src_ref=frames_ref.at[pl.ds(count - 2, 2)],
        dst_ref=halo_one,
        send_sem=halo_send,
        recv_sem=halo_recv,
        device_id={"tm": lax.rem(later, n)},
        device_id_type=MESH,
    )

    def edge_copy(row):
        return pltpu.make_async_remote_copy(
            src_ref=edge_two.at[row],
            dst_ref=halo_two.at[row],
            send_sem=edge_send.at[row],
            recv_sem=edge_recv.at[row],
            device_id={"tm": lax.rem(later, n)},
            device_id_type=MESH,
        )

    @pl.when(later < n)
    def _():
        halo_copy.start()

    for load in loads[1:10]:
        load.wait()
    for load in loads[10:]:
        load.start()

    halves = ROWS // 2
    pairs = count // 2
    steps = pairs * halves
    far = 1 - (2 * me) // n

    def finish(frame, row, conv):
        value = (first[pl.ds(frame, 2), row].astype(jnp.float32) + conv).astype(jnp.bfloat16)
        latent = jnp.dot(
            value.reshape(2 * COLS, channels),
            project[...],
            preferred_element_type=jnp.float32,
        ).astype(jnp.bfloat16)
        for at in range(2):
            for index in range(per_row):
                begin = at * COLS + index * owned
                result[row * per_row + index, frame + at] = latent[begin : begin + owned]

    @pl.loop(0, halves)
    def _(stage):

        @pl.loop(stage * (steps - 1), steps - 1 + stage)
        def _(step):
            frame = count - 2 - 2 * (step // halves)
            near = (far + step) % halves
            head = step == steps - halves

            @pl.when(head & (me > 0))
            def _():
                halo_copy.wait_recv()

                @pl.loop(0, 2 * ROWS)
                def _(index):
                    at = index // ROWS
                    row = index % ROWS
                    store_shifted(acts_one, at, row, norm_act(halo_one[at, row], gain_one[...]))

            @pl.when(head & (me == 0))
            def _():
                @pl.loop(0, 2 * ROWS)
                def _(index):
                    blank = jnp.zeros((COLS, acts_one.shape[-1]), jnp.bfloat16)
                    acts_one[index // ROWS, index % ROWS] = blank
                    acts_two[index // ROWS, index % ROWS] = blank

            for row, conv in both_rows(acts_one, kernel_one, frame, near):
                for at in range(2):
                    value = (frames[frame + at, row].astype(jnp.float32) + conv[at]).astype(
                        jnp.bfloat16
                    )
                    first[frame + at, row] = value
                    store_shifted(acts_two, frame + at + 2, row, norm_act(value, gain_two[...]))

            @pl.when((step < halves) & (later < n))
            def _():
                for row in ((ROWS - 1) * near, 1 + near):
                    for at in range(2):
                        edge_two[row, at] = acts_two[count + at, row, :, channels : 2 * channels]
                    edge_copy(row).start()

        @pl.when(stage == 0)
        def _():
            for load in loads[10:]:
                load.wait()

        @pl.loop(stage * pairs, (3 * stage + 1) * pairs)
        def _(step):
            unit = step // pairs
            frame = count - 2 - 2 * (step % pairs)
            half = (far + unit // 2) % halves
            inner = unit % 2

            @pl.when((step == pairs - 1) & (me > 0))
            def _():
                @pl.loop(0, ROWS)
                def _(row):
                    edge_copy(row).wait_recv()
                    for at in range(2):
                        store_shifted(acts_two, at, row, halo_two[row, at].astype(jnp.float32))

            @pl.when(inner == 0)
            def _():
                conv = conv_row(acts_two, kernel_two, frame, 2 * half, 1 - half, 2)
                finish(frame, (ROWS - 1) * half, conv)

            @pl.when(inner == 1)
            def _():
                finish(frame, 1 + half, conv_row(acts_two, kernel_two, frame, half, 0, 3))

            row = 2 * half + (half + inner) % 2

            @pl.loop(0, per_row)
            def _(index):
                owner = row * per_row + index

                @pl.when(owner != me)
                def _():
                    pltpu.make_async_remote_copy(
                        src_ref=result.at[owner, pl.ds(frame, 2)],
                        dst_ref=out_ref.at[pl.ds(me * count + frame, 2)],
                        send_sem=out_send,
                        recv_sem=out_recv,
                        device_id={"tm": owner},
                        device_id_type=MESH,
                    ).start()

    own = pltpu.make_async_copy(result.at[me], out_ref.at[pl.ds(me * count, count)], own_sem)
    own.start()

    @pl.when(later < n)
    def _():
        halo_copy.wait_send()
        for row in range(ROWS):
            edge_copy(row).wait_send()

    others = out_ref.at[pl.ds(0, (n - 1) * count)]
    sent = result.at[pl.ds(0, n - 1)]
    pltpu.make_async_copy(sent, sent, out_send).wait()
    pltpu.make_async_copy(others, others, out_recv).wait()
    own.wait()


def body(n, frames, gain_one, conv_one, gain_two, conv_two, out_weight):
    count, cells, channels = frames.shape
    owned = cells // n
    grid = (count, ROWS, COLS, channels)
    taps = (9, 3 * channels, channels)
    half = jnp.bfloat16
    hbm = pl.BlockSpec(memory_space=pl.ANY)
    vmem = pl.BlockSpec(memory_space=pltpu.VMEM)
    return pl.pallas_call(
        functools.partial(fused, n),
        out_shape=pltpu.VMEM((n * count, owned, channels), half),
        in_specs=[hbm, vmem, hbm, vmem, hbm, hbm],
        out_specs=hbm,
        scratch_shapes=[
            pltpu.VMEM(grid, half),
            pltpu.VMEM((2, ROWS, COLS, channels), half),
            pltpu.VMEM((ROWS, 2, COLS, channels), half),
            pltpu.VMEM((ROWS, 2, COLS, channels), half),
            pltpu.VMEM(taps, half),
            pltpu.VMEM(taps, half),
            pltpu.VMEM((channels, channels), half),
            pltpu.VMEM((count + 2, ROWS, COLS, 3 * channels), half),
            pltpu.VMEM((count + 2, ROWS, COLS, 3 * channels), half),
            pltpu.VMEM(grid, half),
            pltpu.VMEM((n, count, owned, channels), half),
            pltpu.SemaphoreType.DMA((20,)),
            pltpu.SemaphoreType.DMA,
            pltpu.SemaphoreType.DMA,
            pltpu.SemaphoreType.DMA((ROWS,)),
            pltpu.SemaphoreType.DMA((ROWS,)),
            pltpu.SemaphoreType.DMA,
            pltpu.SemaphoreType.DMA,
            pltpu.SemaphoreType.DMA,
        ],
        compiler_params=pltpu.CompilerParams(collective_id=0, has_side_effects=True),
    )(
        frames.reshape(grid),
        gain_one.reshape(1, channels),
        conv_one.reshape(taps),
        gain_two.reshape(1, channels),
        conv_two.reshape(taps),
        out_weight,
    )


def solution(mesh):
    placed = (P("tm", "clip", None), P(), P(), P(), P(), P())
    return jax.shard_map(
        functools.partial(body, mesh.shape["tm"]),
        mesh=mesh,
        in_specs=placed,
        out_specs=P(None, ("clip", "tm"), None),
        check_vma=False,
    )
```

```python
import functools

import jax
import jax.numpy as jnp
from jax import lax
from jax.experimental import pallas as pl
from jax.experimental.pallas import tpu as pltpu
from jax.sharding import PartitionSpec as P

ROWS = 4
COLS = 128
MESH = pl.DeviceIdType.MESH
DIRECT = ((1, 0), (1, 1), (1, 2), (0, 0), (0, 1), (0, 2), (1, 3), (0, 3))
RELAYED = ((1, 3), (0, 3))
RELAYED_EDGES = (3, 2)


def norm_act(x, half_gain):
    values = x.astype(jnp.float32)
    scale = lax.rsqrt(jnp.mean(values * values, axis=-1, keepdims=True) + 1e-06)
    half = values * scale * half_gain
    return half + half * jnp.tanh(half)


def store_shifted(acts, frame, pos, act):
    channels = act.shape[-1]
    place = lax.broadcasted_iota(jnp.int32, act.shape, 0)
    before = jnp.where(place == 0, 0.0, pltpu.roll(act, 1, 0))
    after = jnp.where(place == COLS - 1, 0.0, pltpu.roll(act, COLS - 1, 0))
    acts[frame, pos, :, :channels] = before.astype(jnp.bfloat16)
    acts[frame, pos, :, channels : 2 * channels] = act.astype(jnp.bfloat16)
    acts[frame, pos, :, 2 * channels :] = after.astype(jnp.bfloat16)


def fused(
    n,
    frames_ref,
    gain_one,
    conv_one,
    gain_two,
    conv_two,
    out_weight,
    out_ref,
    frames,
    halo,
    edges,
    relay,
    kernel_one,
    kernel_two,
    project,
    acts_one,
    acts_two,
    first,
    result,
    frame_sems,
    load_sems,
    halo_send,
    halo_recv,
    edge_send,
    edge_recv,
    relay_send,
    relay_recv,
    out_send,
    out_recv,
    own_sem,
):
    me = lax.axis_index("tm")
    count = frames.shape[0]
    channels = frames.shape[-1]
    owned = result.shape[2]
    per_row = COLS // owned
    later = me + 1
    far = 1 - (2 * me) // n
    sign = 1 - 2 * far
    later_far = 1 - (2 * later) // n
    later_sign = 1 - 2 * later_far
    border = n // 2 - 1
    helper = max(border - 6, 0)

    def row_at(pos):
        return far * (ROWS - 1) + sign * pos

    def at_later(pos):
        return later_far * (ROWS - 1) + later_sign * row_at(pos)

    def from_later(pos):
        return far * (ROWS - 1) + sign * (later_far * (ROWS - 1) + later_sign * pos)

    loads = []
    for pos in range(ROWS):
        loads.append(
            pltpu.make_async_copy(
                frames_ref.at[:, row_at(pos)], frames.at[:, pos], frame_sems.at[pos]
            )
        )
    groups_one = []
    groups_two = []
    for source, target, groups in ((conv_one, kernel_one, groups_one), (conv_two, kernel_two, groups_two)):
        for tap in range(3):
            taps = pl.ds(3 * tap, 3)
            sem = load_sems.at[tap + 3 * (groups is groups_two)]
            groups.append(pltpu.make_async_copy(source.at[taps], target.at[taps], sem))
    project_load = pltpu.make_async_copy(out_weight, project, load_sems.at[6])
    for load in loads:
        load.start()
    for tap in (2, 1, 0):
        groups_one[tap].start()

    barrier = pltpu.get_barrier_semaphore()

    @pl.loop(1, n)
    def _(step):
        pl.semaphore_signal(
            barrier, inc=1, device_id={"tm": lax.rem(me + step, n)}, device_id_type=MESH
        )

    @pl.when(me == 0)
    def _():
        @pl.loop(0, 2 * ROWS)
        def _(index):
            blank = jnp.zeros((COLS, channels), jnp.bfloat16)
            halo[index // ROWS, index % ROWS] = blank
            edges[index // ROWS, index % ROWS] = blank

    gains_one = 0.5 * gain_one[...]
    gains_two = 0.5 * gain_two[...]

    def own_acts(pos):
        for frame in range(count - 1, -1, -1):
            act = norm_act(frames[frame, pos], gains_one)
            store_shifted(acts_one, frame + 2, pos, act)

    def to(device, source, target, send, recv):
        return pltpu.make_async_remote_copy(
            src_ref=source,
            dst_ref=target,
            send_sem=send,
            recv_sem=recv,
            device_id={"tm": lax.rem(device, n)},
            device_id_type=MESH,
        )

    def halo_copy(at, pos):
        source = frames.at[count - 2 + at, from_later(pos)]
        return to(later, source, halo.at[at, pos], halo_send, halo_recv.at[at, pos])

    def halo_to_relay(index):
        at, pos = RELAYED[index]
        source = frames.at[count - 2 + at, from_later(pos)]
        return to(helper, source, relay.at[index], halo_send, relay_recv.at[index])

    def relay_halo(index):
        at, pos = RELAYED[index]
        return to(border + 1, relay.at[index], halo.at[at, pos], relay_send, halo_recv.at[at, pos])

    def edge_source(pos):
        return first.at[pl.ds(count - 2, 2), pos]

    def edge_copy(pos):
        target = at_later(pos)
        return to(later, edge_source(pos), edges.at[:, target], edge_send, edge_recv.at[target])

    def relay_slot(index):
        return relay.at[pl.ds(len(RELAYED) + 2 * index, 2)]

    def edge_to_relay(pos, index):
        recv = relay_recv.at[len(RELAYED) + index]
        return to(helper, edge_source(pos), relay_slot(index), edge_send, recv)

    def relay_edge(index):
        pos = RELAYED_EDGES[index]
        return to(border + 1, relay_slot(index), edges.at[:, pos], relay_send, edge_recv.at[pos])

    def forward(halos, edges):
        @pl.when(me == helper)
        def _():
            for index in halos:
                slot = relay.at[index]
                pltpu.make_async_copy(slot, slot, relay_recv.at[index]).wait()
                relay_halo(index).start()
            for index in edges:
                slot = relay_slot(index)
                pltpu.make_async_copy(slot, slot, relay_recv.at[len(RELAYED) + index]).wait()
                relay_edge(index).start()

    def send_edges(positions):
        @pl.when(me == border)
        def _():
            for pos in positions:
                target = ROWS - 1 - pos
                if target in RELAYED_EDGES:
                    edge_to_relay(pos, RELAYED_EDGES.index(target)).start()
                else:
                    edge_copy(pos).start()

        @pl.when((later < n) & (me != border))
        def _():
            for pos in positions:
                edge_copy(pos).start()

    def conv(acts, kernel, frame, extent, pos, taps=(2, 1, 0), total=None):
        for tap in taps:
            for step in (0, 1, -1):
                if pos + step < 0 or pos + step >= ROWS:
                    continue
                window = acts[pl.ds(frame + tap, extent), pos + step]
                part = jnp.dot(
                    window.reshape(extent * COLS, 3 * channels),
                    kernel[tap * 3 + 1 + step * sign],
                    preferred_element_type=jnp.float32,
                )
                total = part if total is None else total + part
        return total

    pending = []

    def flush():
        for finish in pending:
            finish()
        pending.clear()

    def block(kind, frame, extent, pos):
        finish, acts, kernel = kind
        total = conv(acts, kernel, frame, extent, pos)
        flush()
        pending.append(lambda: finish(total, frame, extent, pos))

    def finish_one(total, frame, extent, pos):
        for at in range(extent):
            part = total[at * COLS : (at + 1) * COLS]
            value = (frames[frame + at, pos].astype(jnp.float32) + part).astype(jnp.bfloat16)
            first[frame + at, pos] = value
            store_shifted(acts_two, frame + at + 2, pos, norm_act(value, gains_two))

    def finish_two(total, frame, extent, pos):
        values = first[pl.ds(frame, extent), pos].reshape(extent * COLS, channels)
        value = (values.astype(jnp.float32) + total).astype(jnp.bfloat16)
        latent = jnp.dot(value, project[...], preferred_element_type=jnp.float32).astype(jnp.bfloat16)
        for at in range(extent):
            for index in range(per_row):
                begin = at * COLS + index * owned
                result[pos * per_row + index, frame + at] = latent[begin : begin + owned]
        own = ROWS // 2 <= pos
        for step in range(own, per_row):
            send(pos, lax.rem(me + step, per_row), frame, extent)

    one = (finish_one, acts_one, kernel_one)
    two = (finish_two, acts_two, kernel_two)

    def send(pos, index, frame, extent):
        to(
            row_at(pos) * per_row + index,
            result.at[pos * per_row + index, pl.ds(frame, extent)],
            out_ref.at[pl.ds(me * count + frame, extent)],
            out_send,
            out_recv,
        ).start()

    def wait_halo(at, positions):
        @pl.when(me > 0)
        def _():
            for pos in positions:
                slot = halo.at[at, pos]
                pltpu.make_async_copy(slot, slot, halo_recv.at[at, pos]).wait()

    def halo_acts(at, positions):
        for pos in positions:
            store_shifted(acts_one, at, pos, norm_act(halo[at, pos], gains_one))

    def wait_edges(positions):
        @pl.when(me > 0)
        def _():
            for pos in positions:
                slot = edges.at[:, pos]
                pltpu.make_async_copy(slot, slot, edge_recv.at[pos]).wait()

    def edge_acts(pos):
        for at in range(2):
            store_shifted(acts_two, at, pos, norm_act(edges[at, pos], gains_two))

    for load in loads:
        load.wait()
    own_acts(0)
    own_acts(1)
    pl.semaphore_wait(barrier, n - 1)

    @pl.when(me == border)
    def _():
        for index in range(len(RELAYED)):
            halo_to_relay(index).start()
        for at, pos in DIRECT:
            if (at, pos) not in RELAYED:
                halo_copy(at, pos).start()

    @pl.when((later < n) & (me != border))
    def _():
        for at, pos in DIRECT:
            halo_copy(at, pos).start()

    for group in groups_one:
        group.wait()
    for group in groups_two:
        group.start()
    project_load.start()

    last = count - 2
    block(one, last, 2, 0)
    own_acts(2)
    block(one, last, 2, 1)
    own_acts(3)
    block(one, last, 2, 2)
    block(one, last, 2, 3)
    flush()
    send_edges(range(ROWS))
    for frame in range(count - 3, -1, -1):
        if frame < 2:
            wait_halo(frame, (0, 1, 2))
            halo_acts(frame, (0, 1, 2))
        block(one, frame, 1, 0)
        block(one, frame, 1, 1)
        if frame == count - 3:
            for group in groups_two:
                group.wait()
            project_load.wait()
        flush()
        block(two, frame + 2, 1, 0)
        flush()
        if frame == count - 3:
            forward(range(len(RELAYED)), ())
    wait_halo(1, (3,))
    wait_halo(0, (3,))
    halo_acts(1, (3,))
    halo_acts(0, (3,))
    for frame in range(count - 4, -1, -2):
        block(one, frame, 2, 2)
    for frame in range(count - 4, -1, -2):
        block(one, frame, 2, 3)
    for frame in range(count - 2, 0, -2):
        block(two, frame, 2, 1)
    flush()
    forward((), range(len(RELAYED_EDGES)))
    wait_edges((0, 1))
    edge_acts(0)
    edge_acts(1)
    block(two, 0, 2, 0)
    for frame in range(count - 2, 0, -2):
        block(two, frame, 2, 2)
    flush()
    wait_edges((2, 3))
    edge_acts(2)
    block(two, 0, 2, 1)
    edge_acts(3)
    for frame in range(count - 2, 0, -2):
        block(two, frame, 2, 3)
    block(two, 0, 2, 2)
    block(two, 0, 2, 3)
    flush()

    for pos in range(ROWS // 2, ROWS):
        index = lax.rem(me, per_row)

        @pl.when(row_at(pos) * per_row + index != me)
        def _():
            send(pos, index, 0, count)

    mine = row_at(lax.rem(me // per_row, ROWS)) * per_row + lax.rem(me, per_row)
    own = pltpu.make_async_copy(
        result.at[mine], out_ref.at[pl.ds(me * count, count)], own_sem
    )
    own.start()

    @pl.when(later < n)
    def _():
        pltpu.make_async_copy(halo, halo, halo_send).wait()
        pltpu.make_async_copy(halo, halo, edge_send).wait()

    @pl.when(me == helper)
    def _():
        pltpu.make_async_copy(relay, relay, relay_send).wait()

    others = out_ref.at[pl.ds(0, (n - 1) * count)]
    sent = result.at[pl.ds(0, n - 1)]
    pltpu.make_async_copy(sent, sent, out_send).wait()
    pltpu.make_async_copy(others, others, out_recv).wait()
    own.wait()


def body(n, frames, gain_one, conv_one, gain_two, conv_two, out_weight):
    count, cells, channels = frames.shape
    owned = cells // n
    grid = (count, ROWS, COLS, channels)
    taps = (9, 3 * channels, channels)
    half = jnp.bfloat16
    hbm = pl.BlockSpec(memory_space=pl.ANY)
    vmem = pl.BlockSpec(memory_space=pltpu.VMEM)
    return pl.pallas_call(
        functools.partial(fused, n),
        out_shape=pltpu.VMEM((n * count, owned, channels), half),
        in_specs=[hbm, vmem, hbm, vmem, hbm, hbm],
        out_specs=hbm,
        scratch_shapes=[
            pltpu.VMEM(grid, half),
            pltpu.VMEM((2, ROWS, COLS, channels), half),
            pltpu.VMEM((2, ROWS, COLS, channels), half),
            pltpu.VMEM((len(RELAYED) + 2 * len(RELAYED_EDGES), COLS, channels), half),
            pltpu.VMEM(taps, half),
            pltpu.VMEM(taps, half),
            pltpu.VMEM((channels, channels), half),
            pltpu.VMEM((count + 2, ROWS, COLS, 3 * channels), half),
            pltpu.VMEM((count + 2, ROWS, COLS, 3 * channels), half),
            pltpu.VMEM(grid, half),
            pltpu.VMEM((n, count, owned, channels), half),
            pltpu.SemaphoreType.DMA((ROWS,)),
            pltpu.SemaphoreType.DMA((7,)),
            pltpu.SemaphoreType.DMA,
            pltpu.SemaphoreType.DMA((2, ROWS)),
            pltpu.SemaphoreType.DMA,
            pltpu.SemaphoreType.DMA((ROWS,)),
            pltpu.SemaphoreType.DMA,
            pltpu.SemaphoreType.DMA((len(RELAYED) + len(RELAYED_EDGES),)),
            pltpu.SemaphoreType.DMA,
            pltpu.SemaphoreType.DMA,
            pltpu.SemaphoreType.DMA,
        ],
        compiler_params=pltpu.CompilerParams(collective_id=0, has_side_effects=True),
    )(
        frames.reshape(grid),
        gain_one.reshape(1, channels),
        conv_one.reshape(taps),
        gain_two.reshape(1, channels),
        conv_two.reshape(taps),
        out_weight,
    )


def solution(mesh):
    placed = (P("tm", "clip", None), P(), P(), P(), P(), P())
    return jax.shard_map(
        functools.partial(body, mesh.shape["tm"]),
        mesh=mesh,
        in_specs=placed,
        out_specs=P(None, ("clip", "tm"), None),
        check_vma=False,
    )
```

```python
import functools

import jax
import jax.numpy as jnp
from jax import lax
from jax.experimental import pallas as pl
from jax.experimental.pallas import tpu as pltpu
from jax.sharding import PartitionSpec as P

ROWS = 4
COLS = 128
MESH = pl.DeviceIdType.MESH
DIRECT = ((1, 0), (1, 1), (1, 2), (0, 0), (0, 1), (0, 2), (1, 3), (0, 3))
RELAYED = ((1, 3), (0, 3))
RELAYED_EDGES = (3,)


def norm_act(x, half_gain):
    values = x.astype(jnp.float32)
    scale = lax.rsqrt(jnp.mean(values * values, axis=-1, keepdims=True) + 1e-06)
    half = values * scale * half_gain
    return half + half * jnp.tanh(half)


def store_shifted(acts, frame, pos, act):
    channels = act.shape[-1]
    place = lax.broadcasted_iota(jnp.int32, act.shape, 0)
    before = jnp.where(place == 0, 0.0, pltpu.roll(act, 1, 0))
    after = jnp.where(place == COLS - 1, 0.0, pltpu.roll(act, COLS - 1, 0))
    acts[frame, pos, :, :channels] = before.astype(jnp.bfloat16)
    acts[frame, pos, :, channels : 2 * channels] = act.astype(jnp.bfloat16)
    acts[frame, pos, :, 2 * channels :] = after.astype(jnp.bfloat16)


def fused(
    n,
    frames_ref,
    gain_one,
    conv_one,
    gain_two,
    conv_two,
    out_weight,
    out_ref,
    frames,
    halo,
    edges,
    relay,
    kernel_one,
    kernel_two,
    project,
    acts_one,
    acts_two,
    first,
    result,
    frame_sems,
    load_sems,
    halo_send,
    halo_recv,
    edge_send,
    edge_recv,
    relay_send,
    relay_recv,
    out_send,
    out_recv,
    own_sem,
):
    me = lax.axis_index("tm")
    count = frames.shape[0]
    channels = frames.shape[-1]
    owned = result.shape[2]
    per_row = COLS // owned
    later = me + 1
    far = 1 - (2 * me) // n
    sign = 1 - 2 * far
    later_far = 1 - (2 * later) // n
    later_sign = 1 - 2 * later_far
    border = n // 2 - 1
    routes = ((border, max(border - 6, 0)), (n // 4 - 1, max(n // 4 - 3, 0)))
    crossing = (me == routes[0][0]) | (me == routes[1][0])

    def row_at(pos):
        return far * (ROWS - 1) + sign * pos

    def at_later(pos):
        return later_far * (ROWS - 1) + later_sign * row_at(pos)

    def from_later(pos):
        return far * (ROWS - 1) + sign * (later_far * (ROWS - 1) + later_sign * pos)

    loads = []
    for pos in range(ROWS):
        loads.append(
            pltpu.make_async_copy(
                frames_ref.at[:, row_at(pos)], frames.at[:, pos], frame_sems.at[pos]
            )
        )
    groups_one = []
    groups_two = []
    for source, target, groups in ((conv_one, kernel_one, groups_one), (conv_two, kernel_two, groups_two)):
        for tap in range(3):
            taps = pl.ds(3 * tap, 3)
            sem = load_sems.at[tap + 3 * (groups is groups_two)]
            groups.append(pltpu.make_async_copy(source.at[taps], target.at[taps], sem))
    project_load = pltpu.make_async_copy(out_weight, project, load_sems.at[6])
    for load in loads:
        load.start()
    for tap in (2, 1, 0):
        groups_one[tap].start()

    barrier = pltpu.get_barrier_semaphore()

    @pl.loop(1, n)
    def _(step):
        pl.semaphore_signal(
            barrier, inc=1, device_id={"tm": lax.rem(me + step, n)}, device_id_type=MESH
        )

    @pl.when(me == 0)
    def _():
        @pl.loop(0, 2 * ROWS)
        def _(index):
            blank = jnp.zeros((COLS, channels), jnp.bfloat16)
            halo[index // ROWS, index % ROWS] = blank
            edges[index // ROWS, index % ROWS] = blank

    gains_one = 0.5 * gain_one[...]
    gains_two = 0.5 * gain_two[...]

    def own_acts(pos):
        for frame in range(count - 1, -1, -1):
            act = norm_act(frames[frame, pos], gains_one)
            store_shifted(acts_one, frame + 2, pos, act)

    def to(device, source, target, send, recv):
        return pltpu.make_async_remote_copy(
            src_ref=source,
            dst_ref=target,
            send_sem=send,
            recv_sem=recv,
            device_id={"tm": lax.rem(device, n)},
            device_id_type=MESH,
        )

    def halo_copy(at, pos):
        source = frames.at[count - 2 + at, from_later(pos)]
        return to(later, source, halo.at[at, pos], halo_send, halo_recv.at[at, pos])

    def halo_to_relay(route, index):
        at, pos = RELAYED[index]
        source = frames.at[count - 2 + at, from_later(pos)]
        recv = relay_recv.at[route, index]
        return to(routes[route][1], source, relay.at[route, index], halo_send, recv)

    def relay_halo(route, index):
        at, pos = RELAYED[index]
        target = routes[route][0] + 1
        recv = halo_recv.at[at, pos]
        return to(target, relay.at[route, index], halo.at[at, pos], relay_send.at[route], recv)

    def edge_source(pos):
        return first.at[pl.ds(count - 2, 2), pos]

    def edge_copy(pos):
        target = at_later(pos)
        return to(later, edge_source(pos), edges.at[:, target], edge_send, edge_recv.at[target])

    def relay_slot(route, index):
        return relay.at[route, pl.ds(len(RELAYED) + 2 * index, 2)]

    def edge_to_relay(route, pos, index):
        recv = relay_recv.at[route, len(RELAYED) + index]
        return to(routes[route][1], edge_source(pos), relay_slot(route, index), edge_send, recv)

    def relay_edge(route, index):
        pos = RELAYED_EDGES[index]
        target = routes[route][0] + 1
        recv = edge_recv.at[pos]
        return to(target, relay_slot(route, index), edges.at[:, pos], relay_send.at[route], recv)

    def forward(halos, edges_at):
        for route in range(len(routes)):

            @pl.when(me == routes[route][1])
            def _():
                for index in halos:
                    slot = relay.at[route, index]
                    pltpu.make_async_copy(slot, slot, relay_recv.at[route, index]).wait()
                    relay_halo(route, index).start()
                for index in edges_at:
                    slot = relay_slot(route, index)
                    recv = relay_recv.at[route, len(RELAYED) + index]
                    pltpu.make_async_copy(slot, slot, recv).wait()
                    relay_edge(route, index).start()

    def send_edges(positions, here=True):
        for route in range(len(routes)):

            @pl.when((me == routes[route][0]) & here)
            def _():
                for pos in positions:
                    target = pos if route else ROWS - 1 - pos
                    if target in RELAYED_EDGES:
                        edge_to_relay(route, pos, RELAYED_EDGES.index(target)).start()
                    else:
                        edge_copy(pos).start()

        @pl.when((later < n) & jnp.logical_not(crossing) & here)
        def _():
            for pos in positions:
                edge_copy(pos).start()

    def conv(acts, kernel, frame, extent, pos, taps=(2, 1, 0), total=None):
        for tap in taps:
            for step in (0, 1, -1):
                if pos + step < 0 or pos + step >= ROWS:
                    continue
                window = acts[pl.ds(frame + tap, extent), pos + step]
                part = jnp.dot(
                    window.reshape(extent * COLS, 3 * channels),
                    kernel[tap * 3 + 1 + step * sign],
                    preferred_element_type=jnp.float32,
                )
                total = part if total is None else total + part
        return total

    pending = []

    def flush():
        for finish in pending:
            finish()
        pending.clear()

    def block(kind, frame, extent, pos):
        finish, acts, kernel = kind
        total = conv(acts, kernel, frame, extent, pos)
        flush()
        pending.append(lambda: finish(total, frame, extent, pos))

    def finish_one(total, frame, extent, pos):
        for at in range(extent):
            part = total[at * COLS : (at + 1) * COLS]
            value = (frames[frame + at, pos].astype(jnp.float32) + part).astype(jnp.bfloat16)
            first[frame + at, pos] = value
            store_shifted(acts_two, frame + at + 2, pos, norm_act(value, gains_two))

    def finish_two(total, frame, extent, pos):
        values = first[pl.ds(frame, extent), pos].reshape(extent * COLS, channels)
        value = (values.astype(jnp.float32) + total).astype(jnp.bfloat16)
        latent = jnp.dot(value, project[...], preferred_element_type=jnp.float32).astype(jnp.bfloat16)
        for at in range(extent):
            for index in range(per_row):
                begin = at * COLS + index * owned
                result[pos * per_row + index, frame + at] = latent[begin : begin + owned]
        own = ROWS // 2 <= pos
        for step in range(own, per_row):
            send(pos, lax.rem(me + step, per_row), frame, extent)

    one = (finish_one, acts_one, kernel_one)
    two = (finish_two, acts_two, kernel_two)

    def send(pos, index, frame, extent):
        to(
            row_at(pos) * per_row + index,
            result.at[pos * per_row + index, pl.ds(frame, extent)],
            out_ref.at[pl.ds(me * count + frame, extent)],
            out_send,
            out_recv,
        ).start()

    def wait_halo(at, positions):
        @pl.when(me > 0)
        def _():
            for pos in positions:
                slot = halo.at[at, pos]
                pltpu.make_async_copy(slot, slot, halo_recv.at[at, pos]).wait()

    def halo_acts(at, positions):
        for pos in positions:
            store_shifted(acts_one, at, pos, norm_act(halo[at, pos], gains_one))

    def wait_edges(positions):
        @pl.when(me > 0)
        def _():
            for pos in positions:
                slot = edges.at[:, pos]
                pltpu.make_async_copy(slot, slot, edge_recv.at[pos]).wait()

    def edge_acts(pos):
        for at in range(2):
            store_shifted(acts_two, at, pos, norm_act(edges[at, pos], gains_two))

    for load in loads:
        load.wait()
    own_acts(0)
    own_acts(1)
    def enter(here):
        @pl.when(here)
        def _():
            pl.semaphore_wait(barrier, n - 1)

        for route in range(len(routes)):

            @pl.when((me == routes[route][0]) & here)
            def _():
                for index in range(len(RELAYED)):
                    halo_to_relay(route, index).start()
                for at, pos in DIRECT:
                    if (at, pos) not in RELAYED:
                        halo_copy(at, pos).start()

        @pl.when((later < n) & jnp.logical_not(crossing) & here)
        def _():
            for at, pos in DIRECT:
                halo_copy(at, pos).start()

    enter(me >= n // 4)

    for group in groups_one:
        group.wait()
    for group in groups_two:
        group.start()
    project_load.start()

    last = count - 2

    def near_blocks(here):
        @pl.when(here)
        def _():
            block(one, last, 2, 2)
            block(one, last, 2, 3)
            flush()

        send_edges((2, 3), here)

    block(one, last, 2, 0)
    own_acts(2)
    block(one, last, 2, 1)
    own_acts(3)
    flush()
    enter(me < n // 4)
    send_edges((0, 1))
    near_blocks(me == border)
    for frame in range(count - 3, -1, -1):
        if frame < 2:
            wait_halo(frame, (0, 1, 2))
            halo_acts(frame, (0, 1, 2))
        block(one, frame, 1, 0)
        block(one, frame, 1, 1)
        if frame == count - 3:
            for group in groups_two:
                group.wait()
            project_load.wait()
        flush()
        block(two, frame + 2, 1, 0)
        flush()
        if frame == count - 3:
            forward(range(len(RELAYED)), ())
    near_blocks(me != border)
    wait_halo(1, (3,))
    wait_halo(0, (3,))
    halo_acts(1, (3,))
    halo_acts(0, (3,))
    for frame in range(count - 4, -1, -2):
        block(one, frame, 2, 2)
    for frame in range(count - 4, -1, -2):
        block(one, frame, 2, 3)
    flush()
    forward((), range(len(RELAYED_EDGES)))
    for frame in range(count - 2, 0, -2):
        block(two, frame, 2, 1)
    flush()
    wait_edges((0, 1))
    edge_acts(0)
    edge_acts(1)
    block(two, 0, 2, 0)
    for pos in (2, 3):
        for frame in range(count - 2, 0, -2):
            block(two, frame, 2, pos)
    flush()
    wait_edges((2, 3))
    edge_acts(2)
    block(two, 0, 2, 1)
    edge_acts(3)
    block(two, 0, 2, 2)
    block(two, 0, 2, 3)
    flush()

    for pos in range(ROWS // 2, ROWS):
        index = lax.rem(me, per_row)

        @pl.when(row_at(pos) * per_row + index != me)
        def _():
            send(pos, index, 0, count)

    mine = row_at(lax.rem(me // per_row, ROWS)) * per_row + lax.rem(me, per_row)
    own = pltpu.make_async_copy(
        result.at[mine], out_ref.at[pl.ds(me * count, count)], own_sem
    )
    own.start()

    @pl.when(later < n)
    def _():
        pltpu.make_async_copy(halo, halo, halo_send).wait()
        pltpu.make_async_copy(halo, halo, edge_send).wait()

    for route in range(len(routes)):

        @pl.when(me == routes[route][1])
        def _():
            pltpu.make_async_copy(relay.at[route], relay.at[route], relay_send.at[route]).wait()

    others = out_ref.at[pl.ds(0, (n - 1) * count)]
    sent = result.at[pl.ds(0, n - 1)]
    pltpu.make_async_copy(sent, sent, out_send).wait()
    pltpu.make_async_copy(others, others, out_recv).wait()
    own.wait()


def body(n, frames, gain_one, conv_one, gain_two, conv_two, out_weight):
    count, cells, channels = frames.shape
    owned = cells // n
    grid = (count, ROWS, COLS, channels)
    taps = (9, 3 * channels, channels)
    half = jnp.bfloat16
    hbm = pl.BlockSpec(memory_space=pl.ANY)
    vmem = pl.BlockSpec(memory_space=pltpu.VMEM)
    return pl.pallas_call(
        functools.partial(fused, n),
        out_shape=pltpu.VMEM((n * count, owned, channels), half),
        in_specs=[hbm, vmem, hbm, vmem, hbm, hbm],
        out_specs=hbm,
        scratch_shapes=[
            pltpu.VMEM(grid, half),
            pltpu.VMEM((2, ROWS, COLS, channels), half),
            pltpu.VMEM((2, ROWS, COLS, channels), half),
            pltpu.VMEM((2, len(RELAYED) + 2 * len(RELAYED_EDGES), COLS, channels), half),
            pltpu.VMEM(taps, half),
            pltpu.VMEM(taps, half),
            pltpu.VMEM((channels, channels), half),
            pltpu.VMEM((count + 2, ROWS, COLS, 3 * channels), half),
            pltpu.VMEM((count + 2, ROWS, COLS, 3 * channels), half),
            pltpu.VMEM(grid, half),
            pltpu.VMEM((n, count, owned, channels), half),
            pltpu.SemaphoreType.DMA((ROWS,)),
            pltpu.SemaphoreType.DMA((7,)),
            pltpu.SemaphoreType.DMA,
            pltpu.SemaphoreType.DMA((2, ROWS)),
            pltpu.SemaphoreType.DMA,
            pltpu.SemaphoreType.DMA((ROWS,)),
            pltpu.SemaphoreType.DMA((2,)),
            pltpu.SemaphoreType.DMA((2, len(RELAYED) + len(RELAYED_EDGES))),
            pltpu.SemaphoreType.DMA,
            pltpu.SemaphoreType.DMA,
            pltpu.SemaphoreType.DMA,
        ],
        compiler_params=pltpu.CompilerParams(collective_id=0, has_side_effects=True),
    )(
        frames.reshape(grid),
        gain_one.reshape(1, channels),
        conv_one.reshape(taps),
        gain_two.reshape(1, channels),
        conv_two.reshape(taps),
        out_weight,
    )


def solution(mesh):
    placed = (P("tm", "clip", None), P(), P(), P(), P(), P())
    return jax.shard_map(
        functools.partial(body, mesh.shape["tm"]),
        mesh=mesh,
        in_specs=placed,
        out_specs=P(None, ("clip", "tm"), None),
        check_vma=False,
    )
```

```python
import functools

import jax
import jax.numpy as jnp
from jax import lax
from jax.experimental import pallas as pl
from jax.experimental.pallas import tpu as pltpu
from jax.sharding import PartitionSpec as P

ROWS = 4
COLS = 128
MESH = pl.DeviceIdType.MESH
DIRECT = ((1, 0), (1, 1), (1, 2), (0, 0), (0, 1), (0, 2), (1, 3), (0, 3))
RELAYED = ((1, 3), (0, 3))
RELAYED_EDGES = (3,)


def norm_act(x, half_gain):
    values = x.astype(jnp.float32)
    scale = lax.rsqrt(jnp.mean(values * values, axis=-1, keepdims=True) + 1e-06)
    half = values * scale * half_gain
    return half + half * jnp.tanh(half)


def store_shifted(acts, frame, pos, act):
    channels = act.shape[-1]
    place = lax.broadcasted_iota(jnp.int32, act.shape, 0)
    before = jnp.where(place == 0, 0.0, pltpu.roll(act, 1, 0))
    after = jnp.where(place == COLS - 1, 0.0, pltpu.roll(act, COLS - 1, 0))
    acts[frame, pos, :, :channels] = before.astype(jnp.bfloat16)
    acts[frame, pos, :, channels : 2 * channels] = act.astype(jnp.bfloat16)
    acts[frame, pos, :, 2 * channels :] = after.astype(jnp.bfloat16)


def fused(
    n,
    frames_ref,
    gain_one,
    conv_one,
    gain_two,
    conv_two,
    out_weight,
    out_ref,
    frames,
    halo,
    edges,
    relay,
    kernel_one,
    kernel_two,
    project,
    acts_one,
    acts_two,
    first,
    result,
    frame_sems,
    load_sems,
    halo_send,
    halo_recv,
    edge_send,
    edge_recv,
    relay_send,
    relay_recv,
    out_send,
    out_recv,
    own_sem,
):
    me = lax.axis_index("tm")
    count = frames.shape[0]
    channels = frames.shape[-1]
    owned = result.shape[2]
    per_row = COLS // owned
    later = me + 1
    far = 1 - (2 * me) // n
    sign = 1 - 2 * far
    later_far = 1 - (2 * later) // n
    later_sign = 1 - 2 * later_far
    border = n // 2 - 1
    routes = ((border, max(border - 6, 0)), (n // 4 - 1, max(n // 4 - 3, 0)))
    crossing = (me == routes[0][0]) | (me == routes[1][0])

    def row_at(pos):
        return far * (ROWS - 1) + sign * pos

    def at_later(pos):
        return later_far * (ROWS - 1) + later_sign * row_at(pos)

    def from_later(pos):
        return far * (ROWS - 1) + sign * (later_far * (ROWS - 1) + later_sign * pos)

    loads = []
    for pos in range(ROWS):
        loads.append(
            pltpu.make_async_copy(
                frames_ref.at[:, row_at(pos)], frames.at[:, pos], frame_sems.at[pos]
            )
        )
    groups_one = []
    groups_two = []
    for source, target, groups in ((conv_one, kernel_one, groups_one), (conv_two, kernel_two, groups_two)):
        for tap in range(3):
            taps = pl.ds(3 * tap, 3)
            sem = load_sems.at[tap + 3 * (groups is groups_two)]
            groups.append(pltpu.make_async_copy(source.at[taps], target.at[taps], sem))
    project_load = pltpu.make_async_copy(out_weight, project, load_sems.at[6])
    for load in loads:
        load.start()
    for tap in (2, 1, 0):
        groups_one[tap].start()

    barrier = pltpu.get_barrier_semaphore()

    @pl.loop(1, n)
    def _(step):
        pl.semaphore_signal(
            barrier, inc=1, device_id={"tm": lax.rem(me + step, n)}, device_id_type=MESH
        )

    @pl.when(me == 0)
    def _():
        @pl.loop(0, 2 * ROWS)
        def _(index):
            blank = jnp.zeros((COLS, channels), jnp.bfloat16)
            halo[index // ROWS, index % ROWS] = blank
            edges[index // ROWS, index % ROWS] = blank

    gains_one = 0.5 * gain_one[...]
    gains_two = 0.5 * gain_two[...]

    def own_acts(pos):
        for frame in range(count - 1, -1, -1):
            act = norm_act(frames[frame, pos], gains_one)
            store_shifted(acts_one, frame + 2, pos, act)

    def to(device, source, target, send, recv):
        return pltpu.make_async_remote_copy(
            src_ref=source,
            dst_ref=target,
            send_sem=send,
            recv_sem=recv,
            device_id={"tm": lax.rem(device, n)},
            device_id_type=MESH,
        )

    def halo_copy(at, pos):
        source = frames.at[count - 2 + at, from_later(pos)]
        return to(later, source, halo.at[at, pos], halo_send, halo_recv.at[at, pos])

    def halo_to_relay(route, index):
        at, pos = RELAYED[index]
        source = frames.at[count - 2 + at, from_later(pos)]
        recv = relay_recv.at[route, index]
        return to(routes[route][1], source, relay.at[route, index], halo_send, recv)

    def relay_halo(route, index):
        at, pos = RELAYED[index]
        target = routes[route][0] + 1
        recv = halo_recv.at[at, pos]
        return to(target, relay.at[route, index], halo.at[at, pos], relay_send.at[route], recv)

    def edge_source(pos):
        return first.at[pl.ds(count - 2, 2), pos]

    def edge_copy(pos):
        target = at_later(pos)
        return to(later, edge_source(pos), edges.at[:, target], edge_send, edge_recv.at[target])

    def relay_slot(route, index):
        return relay.at[route, pl.ds(len(RELAYED) + 2 * index, 2)]

    def edge_to_relay(route, pos, index):
        recv = relay_recv.at[route, len(RELAYED) + index]
        return to(routes[route][1], edge_source(pos), relay_slot(route, index), edge_send, recv)

    def relay_edge(route, index):
        pos = RELAYED_EDGES[index]
        target = routes[route][0] + 1
        recv = edge_recv.at[pos]
        return to(target, relay_slot(route, index), edges.at[:, pos], relay_send.at[route], recv)

    def forward(halos, edges_at):
        for route in range(len(routes)):

            @pl.when(me == routes[route][1])
            def _():
                for index in halos:
                    slot = relay.at[route, index]
                    pltpu.make_async_copy(slot, slot, relay_recv.at[route, index]).wait()
                    relay_halo(route, index).start()
                for index in edges_at:
                    slot = relay_slot(route, index)
                    recv = relay_recv.at[route, len(RELAYED) + index]
                    pltpu.make_async_copy(slot, slot, recv).wait()
                    relay_edge(route, index).start()

    def send_edges(positions, here=True):
        for route in range(len(routes)):

            @pl.when((me == routes[route][0]) & here)
            def _():
                for pos in positions:
                    target = pos if route else ROWS - 1 - pos
                    if target in RELAYED_EDGES:
                        edge_to_relay(route, pos, RELAYED_EDGES.index(target)).start()
                    else:
                        edge_copy(pos).start()

        @pl.when((later < n) & jnp.logical_not(crossing) & here)
        def _():
            for pos in positions:
                edge_copy(pos).start()

    def conv(acts, kernel, frame, extent, pos, arriving=None):
        total = None
        for tap in (2, 1, 0):
            if arriving:
                arriving[tap].wait()
            for step in (0, 1, -1):
                if pos + step < 0 or pos + step >= ROWS:
                    continue
                window = acts[pl.ds(frame + tap, extent), pos + step]
                part = jnp.dot(
                    window.reshape(extent * COLS, 3 * channels),
                    kernel[tap * 3 + 1 + step * sign],
                    preferred_element_type=jnp.float32,
                )
                total = part if total is None else total + part
        return total

    pending = []

    def flush():
        for finish in pending:
            finish()
        pending.clear()

    def block(kind, frame, extent, pos, arriving=None):
        finish, acts, kernel = kind
        total = conv(acts, kernel, frame, extent, pos, arriving)
        flush()
        pending.append(lambda: finish(total, frame, extent, pos))

    def finish_one(total, frame, extent, pos):
        for at in range(extent):
            part = total[at * COLS : (at + 1) * COLS]
            value = (frames[frame + at, pos].astype(jnp.float32) + part).astype(jnp.bfloat16)
            first[frame + at, pos] = value
            store_shifted(acts_two, frame + at + 2, pos, norm_act(value, gains_two))

    def finish_two(total, frame, extent, pos):
        values = first[pl.ds(frame, extent), pos].reshape(extent * COLS, channels)
        value = (values.astype(jnp.float32) + total).astype(jnp.bfloat16)
        latent = jnp.dot(value, project[...], preferred_element_type=jnp.float32).astype(jnp.bfloat16)
        for at in range(extent):
            for index in range(per_row):
                begin = at * COLS + index * owned
                result[pos * per_row + index, frame + at] = latent[begin : begin + owned]
        own = ROWS // 2 <= pos
        for step in range(own, per_row):
            send(pos, lax.rem(me + step, per_row), frame, extent)

    one = (finish_one, acts_one, kernel_one)
    two = (finish_two, acts_two, kernel_two)

    def send(pos, index, frame, extent):
        to(
            row_at(pos) * per_row + index,
            result.at[pos * per_row + index, pl.ds(frame, extent)],
            out_ref.at[pl.ds(me * count + frame, extent)],
            out_send,
            out_recv,
        ).start()

    def wait_halo(at, positions):
        @pl.when(me > 0)
        def _():
            for pos in positions:
                slot = halo.at[at, pos]
                pltpu.make_async_copy(slot, slot, halo_recv.at[at, pos]).wait()

    def halo_acts(at, positions):
        for pos in positions:
            store_shifted(acts_one, at, pos, norm_act(halo[at, pos], gains_one))

    def wait_edges(positions):
        @pl.when(me > 0)
        def _():
            for pos in positions:
                slot = edges.at[:, pos]
                pltpu.make_async_copy(slot, slot, edge_recv.at[pos]).wait()

    def edge_acts(pos):
        for at in range(2):
            store_shifted(acts_two, at, pos, norm_act(edges[at, pos], gains_two))

    for load in loads:
        load.wait()
    own_acts(0)
    own_acts(1)
    def enter(here):
        @pl.when(here)
        def _():
            pl.semaphore_wait(barrier, n - 1)

        for route in range(len(routes)):

            @pl.when((me == routes[route][0]) & here)
            def _():
                for index in range(len(RELAYED)):
                    halo_to_relay(route, index).start()
                for at, pos in DIRECT:
                    if (at, pos) not in RELAYED:
                        halo_copy(at, pos).start()

        @pl.when((later < n) & jnp.logical_not(crossing) & here)
        def _():
            for at, pos in DIRECT:
                halo_copy(at, pos).start()

    enter(me >= n // 4)

    last = count - 2

    def near_blocks(here, positions):
        @pl.when(here)
        def _():
            for pos in positions:
                block(one, last, 2, pos)
            flush()

        send_edges(positions, here)

    block(one, last, 2, 0, groups_one)
    for group in groups_two:
        group.start()
    project_load.start()
    own_acts(2)
    block(one, last, 2, 1)
    own_acts(3)
    flush()
    enter(me < n // 4)
    send_edges((0, 1))
    near_blocks(me == border, (2, 3))
    for frame in range(count - 3, -1, -1):
        if frame < 2:
            wait_halo(frame, (0, 1, 2))
            halo_acts(frame, (0, 1, 2))
        block(one, frame, 1, 0)
        block(one, frame, 1, 1)
        if frame == count - 3:
            for group in groups_two:
                group.wait()
            project_load.wait()
        flush()
        block(two, frame + 2, 1, 0)
        flush()
        if frame == count - 3:
            forward(range(len(RELAYED)), ())
    near_blocks(me != border, (2,))
    wait_halo(1, (3,))
    wait_halo(0, (3,))
    halo_acts(1, (3,))
    halo_acts(0, (3,))
    for frame in range(count - 4, -1, -2):
        block(one, frame, 2, 2)
    flush()
    for frame in range(count - 2, 0, -2):
        block(two, frame, 2, 1)
    flush()
    near_blocks(me != border, (3,))
    for frame in range(count - 4, -1, -2):
        block(one, frame, 2, 3)
    flush()
    forward((), range(len(RELAYED_EDGES)))
    wait_edges((0, 1))
    edge_acts(0)
    edge_acts(1)
    block(two, 0, 2, 0)
    for pos in (2, 3):
        for frame in range(count - 2, 0, -2):
            block(two, frame, 2, pos)
    flush()
    wait_edges((2, 3))
    edge_acts(2)
    block(two, 0, 2, 1)
    edge_acts(3)
    block(two, 0, 2, 2)
    block(two, 0, 2, 3)
    flush()

    for pos in range(ROWS // 2, ROWS):
        index = lax.rem(me, per_row)

        @pl.when(row_at(pos) * per_row + index != me)
        def _():
            send(pos, index, 0, count)

    mine = row_at(lax.rem(me // per_row, ROWS)) * per_row + lax.rem(me, per_row)
    own = pltpu.make_async_copy(
        result.at[mine], out_ref.at[pl.ds(me * count, count)], own_sem
    )
    own.start()

    @pl.when(later < n)
    def _():
        pltpu.make_async_copy(halo, halo, halo_send).wait()
        pltpu.make_async_copy(halo, halo, edge_send).wait()

    for route in range(len(routes)):

        @pl.when(me == routes[route][1])
        def _():
            pltpu.make_async_copy(relay.at[route], relay.at[route], relay_send.at[route]).wait()

    others = out_ref.at[pl.ds(0, (n - 1) * count)]
    sent = result.at[pl.ds(0, n - 1)]
    pltpu.make_async_copy(sent, sent, out_send).wait()
    pltpu.make_async_copy(others, others, out_recv).wait()
    own.wait()


def body(n, frames, gain_one, conv_one, gain_two, conv_two, out_weight):
    count, cells, channels = frames.shape
    owned = cells // n
    grid = (count, ROWS, COLS, channels)
    taps = (9, 3 * channels, channels)
    half = jnp.bfloat16
    hbm = pl.BlockSpec(memory_space=pl.ANY)
    vmem = pl.BlockSpec(memory_space=pltpu.VMEM)
    return pl.pallas_call(
        functools.partial(fused, n),
        out_shape=pltpu.VMEM((n * count, owned, channels), half),
        in_specs=[hbm, vmem, hbm, vmem, hbm, hbm],
        out_specs=hbm,
        scratch_shapes=[
            pltpu.VMEM(grid, half),
            pltpu.VMEM((2, ROWS, COLS, channels), half),
            pltpu.VMEM((2, ROWS, COLS, channels), half),
            pltpu.VMEM((2, len(RELAYED) + 2 * len(RELAYED_EDGES), COLS, channels), half),
            pltpu.VMEM(taps, half),
            pltpu.VMEM(taps, half),
            pltpu.VMEM((channels, channels), half),
            pltpu.VMEM((count + 2, ROWS, COLS, 3 * channels), half),
            pltpu.VMEM((count + 2, ROWS, COLS, 3 * channels), half),
            pltpu.VMEM(grid, half),
            pltpu.VMEM((n, count, owned, channels), half),
            pltpu.SemaphoreType.DMA((ROWS,)),
            pltpu.SemaphoreType.DMA((7,)),
            pltpu.SemaphoreType.DMA,
            pltpu.SemaphoreType.DMA((2, ROWS)),
            pltpu.SemaphoreType.DMA,
            pltpu.SemaphoreType.DMA((ROWS,)),
            pltpu.SemaphoreType.DMA((2,)),
            pltpu.SemaphoreType.DMA((2, len(RELAYED) + len(RELAYED_EDGES))),
            pltpu.SemaphoreType.DMA,
            pltpu.SemaphoreType.DMA,
            pltpu.SemaphoreType.DMA,
        ],
        compiler_params=pltpu.CompilerParams(collective_id=0, has_side_effects=True),
    )(
        frames.reshape(grid),
        gain_one.reshape(1, channels),
        conv_one.reshape(taps),
        gain_two.reshape(1, channels),
        conv_two.reshape(taps),
        out_weight,
    )


def solution(mesh):
    placed = (P("tm", "clip", None), P(), P(), P(), P(), P())
    return jax.shard_map(
        functools.partial(body, mesh.shape["tm"]),
        mesh=mesh,
        in_specs=placed,
        out_specs=P(None, ("clip", "tm"), None),
        check_vma=False,
    )
```
